32 devices in a mesh: gx: 2 (over y), gy: 4 (over z), gz: 4 (over x, core).
Axes of the slice: x: 2, y: 2, z: 4, core: 2. Of those that a mesh axis runs over, the one named last changes fastest.
Arguments:
- kinematics: float32 [18, 8192], P(None, ('gx', 'gy', 'gz')), may hold values from -6 to 6
- pair_offsets: float32 [3, 16, 8192], P(None, None, ('gx', 'gy', 'gz')), may hold values from -1 to 1
- pair_index: int32 [16, 8192], P(None, ('gx', 'gy', 'gz')), may hold values from 0 to 687, as said below
- neighbour_count: int32 [8192], P(('gx', 'gy', 'gz')), may hold values from 1 to 16
- send_rows: int32 [27, 512], P(None, ('gx', 'gy', 'gz')), may hold values from 0 to 255
- migrate_dir: int32 [8192], P(('gx', 'gy', 'gz')), may hold values from 0 to 26, as said below
- migrate_slot: int32 [8192], P(('gx', 'gy', 'gz')), may hold values from 0 to 3, as said below
- enc_node_w1: float32 [15, 128], replicated, may hold values from -1.5 to 1.5
- enc_node_w2: bfloat16 [128, 128], replicated, may hold values from -0.5 to 0.5
- enc_edge_w1: float32 [4, 128], replicated, may hold values from -3 to 3
- enc_edge_w2: bfloat16 [128, 128], replicated, may hold values from -0.5 to 0.5
- edge_w1: bfloat16 [3, 384, 128], replicated, may hold values from -0.3125 to 0.3125
- edge_w2: bfloat16 [3, 128, 128], replicated, may hold values from -0.5 to 0.5
- node_w1: bfloat16 [3, 256, 128], replicated, may hold values from -0.375 to 0.375
- node_w2: bfloat16 [3, 128, 128], replicated, may hold values from -0.5 to 0.5
- edge_gain: float32 [3, 128], replicated, may hold values from 0.25 to 1.75
- node_gain: float32 [3, 128], replicated, may hold values from 0.25 to 1.75
- dec_w1: bfloat16 [128, 128], replicated, may hold values from -0.5 to 0.5
- dec_w2: float32 [3, 128], replicated, may hold values from -0.5 to 0.5
Outputs:
- stayed: float32 [18, 8192], P(None, ('gx', 'gy', 'gz'))
- arrived: float32 [18, 3456], P(None, ('gx', 'gy', 'gz'))
The draws below stay inside these ranges and needn't reach their ends.
Inputs may be any that keep to these rules, and one draw needn't show every extreme that they name: `pair_index`: A value below 256 names a row of the particle's own subdomain. A value v of 256 or more names ghost row v - 256; its direction (v - 256) // 16 is never 13 and points to a subdomain inside the grid. How many ghost rows of a direction are named differs between directions and subdomains. `migrate_dir`: A value other than 13 points to a subdomain inside the grid. On one subdomain at most 4 particles share a direction, and on every subdomain some direction has exactly 4. `migrate_slot`: among the particles of one subdomain that leave in one direction the slots are distinct; for staying particles the slot means nothing.
All inputs are finite; a program needn't handle non-finite values.
Results may differ from the reference program's by a relative error of at most 0.0085.
Values may be sent and summed in bfloat16 or wider, within the bound.
A program may use at most 64 MiB of HBM per device.

```python
import jax
import jax.numpy as jnp
import numpy as np
from jax import lax

LATENT = 128
HIDDEN_SIZE = 128
PART_DEV = 256
K = 16
GHOST = 16
MIG = 4
ROUNDS = 3
STATE = 18
PARTICLES = 8192
SENDS = 512
N_GX = 2
N_GY = 4
N_GZ = 4


def inside_table():
    device_total = N_GX * N_GY * N_GZ
    direction = np.arange(27)
    shifts = np.stack([direction // 9 - 1, direction // 3 % 3 - 1, direction % 3 - 1], axis=1)
    device = jnp.arange(device_total, dtype=jnp.int32)[:, None]
    along_first = device // (N_GY * N_GZ) + jnp.asarray(shifts[:, 0], jnp.int32)[None, :]
    along_second = device // N_GZ % N_GY + jnp.asarray(shifts[:, 1], jnp.int32)[None, :]
    along_third = device % N_GZ + jnp.asarray(shifts[:, 2], jnp.int32)[None, :]
    inside = (along_first >= 0) & (along_first < N_GX) & (along_second >= 0) & (along_second < N_GY) & (along_third >= 0) & (along_third < N_GZ)
    inside = inside & jnp.asarray(direction != 13)[None, :]
    kind_table = jnp.asarray(np.abs(shifts).sum(axis=1), jnp.int32)
    return (inside, kind_table)


def valid_order(inside):
    ranking = jnp.where(inside, 0, 1) * 32 + jnp.arange(27, dtype=jnp.int32)[None, :]
    ordered = jnp.argsort(ranking, axis=1).astype(jnp.int32)
    return (ordered, jnp.sum(inside.astype(jnp.int32), axis=1))


def draw_pair_index(key, part):
    device_total = N_GX * N_GY * N_GZ
    inside, kind_table = inside_table()
    ordered, valid_total = valid_order(inside)
    subkeys = jax.random.split(jax.random.fold_in(key, 11), 8)
    face_fill = jax.random.randint(subkeys[0], (device_total, 27), 3 * GHOST // 4, GHOST + 1)
    edge_fill = jax.random.randint(subkeys[1], (device_total, 27), GHOST // 2, GHOST + 1)
    corner_fill = jax.random.randint(subkeys[2], (device_total, 27), GHOST // 2, GHOST + 1)
    filled = jnp.where(kind_table[None, :] == 1, face_fill, jnp.where(kind_table[None, :] == 2, edge_fill, corner_fill))
    heavy_pick = jax.random.randint(subkeys[3], (device_total,), 0, valid_total)
    heavy_dir = jnp.take_along_axis(ordered, heavy_pick[:, None], axis=1)
    filled = jnp.where(jnp.arange(27, dtype=jnp.int32)[None, :] == heavy_dir, GHOST, filled)
    draw_shape = (K, device_total, PART_DEV)
    ghostly = jax.random.randint(subkeys[4], draw_shape, 0, 10) < 3
    local_row = jax.random.randint(subkeys[5], draw_shape, 0, PART_DEV)
    device = jnp.arange(device_total, dtype=jnp.int32)[None, :, None]
    picked_rank = jax.random.randint(subkeys[6], draw_shape, 0, valid_total[None, :, None])
    direction = ordered[device, picked_rank]
    slot_index = jax.random.randint(subkeys[7], draw_shape, 0, filled[device, direction])
    entries = jnp.where(ghostly, PART_DEV + direction * GHOST + slot_index, local_row)
    return entries.reshape(K, device_total * PART_DEV).astype(jnp.int32)


def migration_plan(key):
    device_total = N_GX * N_GY * N_GZ
    inside, kind_table = inside_table()
    ordered, valid_total = valid_order(inside)
    subkeys = jax.random.split(jax.random.fold_in(key, 23), 4)
    taken = jax.random.randint(subkeys[0], (device_total, 27), 0, MIG + 1)
    taken = jnp.where(inside, taken, 0)
    heavy_pick = jax.random.randint(subkeys[1], (device_total,), 0, valid_total)
    heavy_dir = jnp.take_along_axis(ordered, heavy_pick[:, None], axis=1)
    taken = jnp.where(jnp.arange(27, dtype=jnp.int32)[None, :] == heavy_dir, MIG, taken)
    permuted = jax.vmap(lambda subkey: jax.random.permutation(subkey, PART_DEV))(jax.random.split(subkeys[2], device_total))
    ranks = jnp.argsort(permuted, axis=1).astype(jnp.int32)
    direction = jnp.minimum(ranks // MIG, 26)
    slot_index = ranks % MIG
    device = jnp.arange(device_total, dtype=jnp.int32)[:, None]
    leaving = (ranks < 27 * MIG) & (slot_index < taken[device, direction])
    spare = jax.random.randint(subkeys[3], (device_total, PART_DEV), 0, MIG)
    targets = jnp.where(leaving, direction, 13)
    slots_out = jnp.where(leaving, slot_index, spare)
    return (targets.reshape(-1).astype(jnp.int32), slots_out.reshape(-1).astype(jnp.int32))


def draw_migrate_dir(key, part):
    return migration_plan(key)[0]


def draw_migrate_slot(key, part):
    return migration_plan(key)[1]


def plant(array, rng, low, top_value):
    spot = [jax.random.randint(jax.random.fold_in(rng, axis), (), 0, length) for axis, length in enumerate(array.shape)]
    main_axis = array.shape.index(max(array.shape))
    next_to = spot[:main_axis] + [(spot[main_axis] + 1) % array.shape[main_axis]] + spot[main_axis + 1:]
    return array.at[tuple(spot)].set(low).at[tuple(next_to)].set(top_value)


def level_of(key, extent, cuts, smallest, top_value):
    gain = 1.0
    for axis_at, blocks in cuts:
        draws = jax.random.uniform(jax.random.fold_in(jax.random.fold_in(key, 6), axis_at), (blocks,), jnp.float32, smallest / len(cuts), top_value / len(cuts))
        gain = gain * jnp.repeat(jnp.exp(draws), extent[axis_at] // blocks).reshape((-1,) + (1,) * (len(extent) - 1 - axis_at))
    return gain


def centred(stream_key, shape, deviation, reach, cuts=(), held_as=jnp.bfloat16):
    array = deviation * jax.random.normal(stream_key, shape, jnp.float32)
    if cuts:
        array = array * level_of(stream_key, shape, cuts, -0.22, 0.18)
    return jnp.clip(array, -reach, reach).astype(held_as)


def setup_inputs(seed: int = 0) -> dict:
    keys = jax.random.split(jax.random.key(seed), 20)
    return {
        "kinematics": centred(keys[0], (STATE, PARTICLES), 1.0, 6.0, ((1, 32),), jnp.float32),
        "pair_offsets": jnp.clip(jax.random.uniform(keys[1], (3, K, PARTICLES), jnp.float32, -1.0, 1.0) * level_of(keys[1], (3, K, PARTICLES), ((2, 32),), -0.4, 0.0), -1.0, 1.0),
        "pair_index": draw_pair_index(jax.random.fold_in(keys[19], 71), 0),
        "neighbour_count": plant(jax.random.randint(keys[3], (PARTICLES,), 1, K + 1), jax.random.fold_in(keys[3], 1), 1, K).astype(jnp.int32),
        "send_rows": plant(jax.random.randint(keys[4], (27, SENDS), 0, PART_DEV), jax.random.fold_in(keys[4], 1), 0, PART_DEV - 1).astype(jnp.int32),
        "migrate_dir": draw_migrate_dir(jax.random.fold_in(keys[19], 71), 0),
        "migrate_slot": draw_migrate_slot(jax.random.fold_in(keys[19], 71), 0),
        "enc_node_w1": centred(keys[7], (STATE - 3, HIDDEN_SIZE), (STATE - 3) ** -0.5, 1.5, (), jnp.float32),
        "enc_node_w2": centred(keys[8], (HIDDEN_SIZE, LATENT), HIDDEN_SIZE ** -0.5, 0.5),
        "enc_edge_w1": centred(keys[9], (4, HIDDEN_SIZE), 4 ** -0.5, 3.0, (), jnp.float32),
        "enc_edge_w2": centred(keys[10], (HIDDEN_SIZE, LATENT), HIDDEN_SIZE ** -0.5, 0.5),
        "edge_w1": centred(keys[11], (ROUNDS, 3 * LATENT, HIDDEN_SIZE), (3 * LATENT) ** -0.5, 0.3125),
        "edge_w2": centred(keys[12], (ROUNDS, HIDDEN_SIZE, LATENT), HIDDEN_SIZE ** -0.5, 0.5),
        "node_w1": centred(keys[13], (ROUNDS, 2 * LATENT, HIDDEN_SIZE), (2 * LATENT) ** -0.5, 0.375),
        "node_w2": centred(keys[14], (ROUNDS, HIDDEN_SIZE, LATENT), HIDDEN_SIZE ** -0.5, 0.5),
        "edge_gain": jnp.clip(1.0 + 0.15 * jax.random.normal(keys[15], (ROUNDS, LATENT), jnp.float32), 0.25, 1.75),
        "node_gain": jnp.clip(1.0 + 0.15 * jax.random.normal(keys[16], (ROUNDS, LATENT), jnp.float32), 0.25, 1.75),
        "dec_w1": centred(keys[17], (LATENT, HIDDEN_SIZE), LATENT ** -0.5, 0.5),
        "dec_w2": centred(keys[18], (3, HIDDEN_SIZE), HIDDEN_SIZE ** -0.5, 0.5, (), jnp.float32),
    }


norm_eps = 1e-05

def layer_norm(values):
    center = values - lax.optimization_barrier(jnp.mean(values, axis=-1, keepdims=True))
    spread = lax.optimization_barrier(jnp.mean(center * center, axis=-1, keepdims=True))
    return center * lax.rsqrt(spread + norm_eps)

def encode_edges(offsets, first_weight, second_weight):
    squared = lax.optimization_barrier(jnp.sum(offsets * offsets, axis=0, keepdims=True))
    features = jnp.concatenate([offsets, squared], axis=0)
    hidden = jnp.maximum(jnp.einsum('ckp,ch->kph', features, first_weight, precision=lax.Precision.HIGHEST), 0.0).astype(jnp.bfloat16)
    pair_slots, particles, inner_width = hidden.shape
    result = jnp.dot(hidden.reshape(pair_slots * particles, inner_width), second_weight, preferred_element_type=jnp.float32)
    return layer_norm(result).astype(jnp.bfloat16).reshape(pair_slots, particles, second_weight.shape[1])

def message_round(latent, extended, edge_latent, pair_index, neighbour_count, edge_first, edge_second, node_first, node_second, edge_scale, node_scale, block_pairs):
    latent_width = latent.shape[1]
    pair_slots, particles = pair_index.shape
    sender_proj = jnp.dot(extended, edge_first[2 * latent_width:], preferred_element_type=jnp.float32)
    receiver_proj = jnp.dot(latent, edge_first[latent_width:2 * latent_width], preferred_element_type=jnp.float32)
    summed = jnp.zeros((particles, edge_second.shape[1]), jnp.float32)
    for first_pair in range(0, pair_slots, block_pairs):
        chosen = pair_index[first_pair:first_pair + block_pairs]
        edge_rows = edge_latent[first_pair:first_pair + block_pairs].reshape(block_pairs * particles, latent_width)
        pre_act = jnp.dot(edge_rows, edge_first[:latent_width], preferred_element_type=jnp.float32).reshape(block_pairs, particles, -1)
        pre_act = pre_act + receiver_proj[None] + sender_proj[chosen]
        hidden = jnp.maximum(pre_act, 0.0).astype(jnp.bfloat16)
        message = layer_norm(jnp.dot(hidden.reshape(block_pairs * particles, -1), edge_second, preferred_element_type=jnp.float32)) * edge_scale
        message = message.reshape(block_pairs, particles, -1)
        usable = (first_pair + jnp.arange(block_pairs, dtype=jnp.int32))[:, None] < neighbour_count[None, :]
        summed = summed + lax.optimization_barrier(jnp.sum(jnp.where(usable[:, :, None], message, 0.0), axis=0))
    aggregate = summed.astype(jnp.bfloat16)
    node_pre = jnp.dot(latent, node_first[:latent_width], preferred_element_type=jnp.float32) + jnp.dot(aggregate, node_first[latent_width:], preferred_element_type=jnp.float32)
    node_mid = jnp.maximum(node_pre, 0.0).astype(jnp.bfloat16)
    update = layer_norm(jnp.dot(node_mid, node_second, preferred_element_type=jnp.float32)) * node_scale
    return (latent.astype(jnp.float32) + update).astype(jnp.bfloat16)

def direction_table():
    direction = np.arange(27)
    return np.stack([direction // 9 - 1, direction // 3 % 3 - 1, direction % 3 - 1], axis=1)

def neighbour_ids(device):
    shifts = jnp.asarray(direction_table(), dtype=jnp.int32)
    along_first = device // (N_GY * N_GZ) + shifts[:, 0]
    along_second = device // N_GZ % N_GY + shifts[:, 1]
    along_third = device % N_GZ + shifts[:, 2]
    inside = (along_first >= 0) & (along_first < N_GX) & (along_second >= 0) & (along_second < N_GY) & (along_third >= 0) & (along_third < N_GZ)
    other_id = (jnp.clip(along_first, 0, N_GX - 1) * N_GY + jnp.clip(along_second, 0, N_GY - 1)) * N_GZ + jnp.clip(along_third, 0, N_GZ - 1)
    return (other_id.astype(jnp.int32), inside)

def reference(kinematics, pair_offsets, pair_index, neighbour_count, send_rows, migrate_dir, migrate_slot, enc_node_w1, enc_node_w2, enc_edge_w1, enc_edge_w2, edge_w1, edge_w2, node_w1, node_w2, edge_gain, node_gain, dec_w1, dec_w2):
    device_total = N_GX * N_GY * N_GZ
    latent_width = enc_node_w2.shape[1]
    node_hidden = jnp.maximum(jnp.einsum('cn,ch->nh', kinematics[3:], enc_node_w1, precision=lax.Precision.HIGHEST), 0.0).astype(jnp.bfloat16)
    latent = layer_norm(jnp.dot(node_hidden, enc_node_w2, preferred_element_type=jnp.float32)).astype(jnp.bfloat16)
    latent = latent.reshape(device_total, PART_DEV, latent_width)
    offsets_split = pair_offsets.reshape(3, K, device_total, PART_DEV)
    pairs_split = pair_index.reshape(K, device_total, PART_DEV)
    counts_split = neighbour_count.reshape(device_total, PART_DEV)
    sends_split = send_rows.reshape(27, device_total, GHOST)
    backward = (26 - jnp.arange(27, dtype=jnp.int32)).astype(jnp.int32)
    for round_index in range(ROUNDS):

        def advance(device, latent=latent, round_index=round_index):
            other_id, inside = neighbour_ids(device)
            picked = sends_split[backward, other_id]
            ghosts = latent[other_id[:, None], picked]
            ghosts = jnp.where(inside[:, None, None], ghosts, jnp.zeros_like(ghosts))
            extended = jnp.concatenate([latent[device], ghosts.reshape(27 * GHOST, latent_width)], axis=0)
            edge_latent = encode_edges(offsets_split[:, :, device], enc_edge_w1, enc_edge_w2)
            return message_round(latent[device], extended, edge_latent, pairs_split[:, device], counts_split[device], edge_w1[round_index], edge_w2[round_index], node_w1[round_index], node_w2[round_index], edge_gain[round_index], node_gain[round_index], K)
        latent = lax.map(advance, jnp.arange(device_total, dtype=jnp.int32))
    flat_latent = latent.reshape(device_total * PART_DEV, latent_width)
    decode_hidden = jnp.maximum(jnp.dot(flat_latent, dec_w1, preferred_element_type=jnp.float32), 0.0).astype(jnp.bfloat16)
    acceleration = jnp.einsum('ch,nh->cn', dec_w2, decode_hidden.astype(jnp.float32), precision=lax.Precision.HIGHEST)
    velocity = kinematics[STATE - 3:] + acceleration
    new_state = jnp.concatenate([kinematics[:3] + velocity, kinematics[6:], velocity], axis=0)
    staying = migrate_dir == 13
    stayed = jnp.where(staying[None, :], new_state, 0.0)
    owner_device = (jnp.arange(device_total * PART_DEV, dtype=jnp.int32) // PART_DEV).astype(jnp.int32)
    target = jnp.where(staying, 27, migrate_dir).astype(jnp.int32)
    mailbox = jnp.zeros((device_total, 28, MIG, STATE), jnp.float32).at[owner_device, target, migrate_slot.astype(jnp.int32)].set(new_state.T)
    other_all, inside_all = jax.vmap(neighbour_ids)(jnp.arange(device_total, dtype=jnp.int32))
    received = mailbox[other_all, backward[None, :]]
    received = jnp.where(inside_all[:, :, None, None], received, 0.0)
    arrived = received.reshape(device_total * 27 * MIG, STATE).T
    return (stayed, arrived)
```

```python
import functools

import jax
import jax.numpy as jnp
from jax import lax
from jax.experimental import pallas as pl
from jax.experimental.pallas import tpu as pltpu
from jax.sharding import PartitionSpec as P

MIG = 4
SLOT_ROWS = 8
KERNEL_EXCHANGE = True

norm_eps = 1e-05
F32 = jnp.float32
BF16 = jnp.bfloat16
HIGHEST = lax.Precision.HIGHEST
MESH = pl.DeviceIdType.MESH
AXES = ("gx", "gy", "gz")


def dot(a, b, precision=None):
    return jnp.dot(a, b, preferred_element_type=F32, precision=precision)


def dot_nt(a, b, precision=None):
    return lax.dot_general(
        a, b, (((1,), (1,)), ((), ())), preferred_element_type=F32, precision=precision
    )


def turned(weight):
    return weight.astype(F32).T.astype(weight.dtype)


def normed(values):
    center = values - jnp.mean(values, axis=0, keepdims=True)
    spread = jnp.mean(center * center, axis=0, keepdims=True)
    return center, lax.rsqrt(spread + norm_eps)


def as_column(row, lanes):
    width = row.shape[1]
    square = jnp.broadcast_to(row, (width, width)).T
    return jnp.broadcast_to(square[:, 0:1], (width, lanes))


def fill_outbox(send_hot, latent, outbox_ref):
    outbox_ref[...] = dot_nt(send_hot, latent).astype(BF16).reshape(outbox_ref.shape)


def encode_kernel(
    kin_ref,
    off_ref,
    send_ref,
    node_w1,
    node_w2,
    edge_w1,
    edge_w2,
    latent_ref,
    edge_ref,
    hot_ref,
    outbox_ref,
    square,
    wide,
    columns,
):
    width = node_w2.shape[1]
    particles = kin_ref.shape[1]
    pair_slots = off_ref.shape[1]
    directions, ghost_count = send_ref.shape
    features = node_w1.shape[0]
    square[...] = jnp.zeros_like(square)
    wide[...] = jnp.zeros_like(wide)
    square[0:features, :] = node_w1[...]
    wide[0:features, :] = kin_ref[3:, :]
    hidden = jnp.maximum(dot(square[...].T, wide[...], HIGHEST), 0.0).astype(BF16)
    center, scale = normed(dot(turned(node_w2[...]), hidden))
    latent = (center * scale).astype(BF16)
    latent_ref[...] = latent

    rows = lax.broadcasted_iota(jnp.int32, (ghost_count, ghost_count), 0)
    lanes = lax.broadcasted_iota(jnp.int32, (ghost_count, ghost_count), 1)
    unit = (rows == lanes).astype(F32)
    wanted = dot_nt(unit, send_ref[...].astype(F32), HIGHEST)
    position = lax.broadcasted_iota(jnp.int32, (ghost_count, particles), 1).astype(F32)
    for q in range(directions):
        near = jnp.abs(wanted[:, q : q + 1] - position) < 0.5
        hot_ref[q * ghost_count : (q + 1) * ghost_count, :] = jnp.where(near, 1.0, 0.0).astype(BF16)
    fill_outbox(hot_ref[...], latent, outbox_ref)

    square[0:4, :] = edge_w1[...]
    first = square[...].T
    for c in range(4):
        columns[c] = jnp.broadcast_to(first[:, c : c + 1], (width, particles))
    second = turned(edge_w2[...])

    def one_slot(k, carry):
        x = off_ref[0, pl.ds(k, 1), :]
        y = off_ref[1, pl.ds(k, 1), :]
        z = off_ref[2, pl.ds(k, 1), :]
        pre = columns[0] * x + columns[1] * y + columns[2] * z
        pre = pre + columns[3] * (x * x + y * y + z * z)
        mid = jnp.maximum(pre, 0.0).astype(BF16)
        center, scale = normed(dot(second, mid))
        edge_ref[k] = (center * scale).astype(BF16)
        return carry

    lax.fori_loop(0, pair_slots, one_slot, 0, unroll=4)


def update_latent(
    latent_ref, ghost_ref, edge_ref, index_ref, count_ref, edge_w1, edge_w2, node_w1, node_w2,
    edge_gain, node_gain, extended, joined,
):
    width, particles = latent_ref.shape
    pair_slots = index_ref.shape[0]
    ghosts = ghost_ref[...].reshape(-1, width)
    rows = particles + ghosts.shape[0]
    latent = latent_ref[...]
    diagonal = lax.broadcasted_iota(jnp.int32, (width, width), 0) == lax.broadcasted_iota(
        jnp.int32, (width, width), 1
    )
    unit = jnp.where(diagonal, 1.0, 0.0).astype(BF16)
    extended[:, :particles] = latent
    extended[:, particles:] = dot_nt(unit, ghosts).astype(BF16)
    joined[:, :width] = turned(edge_w1[:width, :])
    joined[:, width:] = turned(edge_w1[2 * width :, :])
    received = dot(turned(edge_w1[width : 2 * width, :]), latent)
    second = turned(edge_w2[...])
    row_id = lax.broadcasted_iota(jnp.int32, (rows, particles), 0)
    count = count_ref[...]

    def one_slot(k, total):
        hot = jnp.where(row_id == index_ref[pl.ds(k, 1), :], 1.0, 0.0).astype(BF16)
        sender = dot(extended[...], hot).astype(BF16)
        both = jnp.concatenate([edge_ref[k], sender], axis=0)
        hidden = jnp.maximum(dot(joined[...], both) + received, 0.0).astype(BF16)
        center, scale = normed(dot(second, hidden))
        return total + center * jnp.where(k < count, scale, 0.0)

    total = lax.fori_loop(
        0, pair_slots, one_slot, jnp.zeros((width, particles), F32), unroll=4
    )
    aggregate = (total * as_column(edge_gain[...], particles)).astype(BF16)
    pre = dot(turned(node_w1[:width, :]), latent) + dot(turned(node_w1[width:, :]), aggregate)
    center, scale = normed(dot(turned(node_w2[...]), jnp.maximum(pre, 0.0).astype(BF16)))
    update = center * scale * as_column(node_gain[...], particles)
    return (latent.astype(F32) + update).astype(BF16)


def round_kernel(
    latent_ref, ghost_ref, edge_ref, index_ref, count_ref, hot_ref, edge_w1, edge_w2, node_w1,
    node_w2, edge_gain, node_gain, latent_out, outbox_ref, extended, joined,
):
    latent = update_latent(
        latent_ref, ghost_ref, edge_ref, index_ref, count_ref, edge_w1, edge_w2, node_w1, node_w2,
        edge_gain, node_gain, extended, joined,
    )
    latent_out[...] = latent
    fill_outbox(hot_ref[...], latent, outbox_ref)


def last_kernel(
    latent_ref, ghost_ref, edge_ref, index_ref, count_ref, edge_w1, edge_w2, node_w1, node_w2,
    edge_gain, node_gain, kin_ref, dir_ref, slot_ref, dec_w1, dec_w2, stayed_ref, leaving_ref,
    extended, joined, state, reading,
):
    latent = update_latent(
        latent_ref, ghost_ref, edge_ref, index_ref, count_ref, edge_w1, edge_w2, node_w1, node_w2,
        edge_gain, node_gain, extended, joined,
    )
    state_rows, particles = kin_ref.shape
    hidden = jnp.maximum(dot(turned(dec_w1[...]), latent), 0.0).astype(BF16)
    reading[...] = jnp.zeros_like(reading)
    reading[0:3, :] = dec_w2[...]
    acceleration = dot(reading[...], hidden.astype(F32), HIGHEST)[0:3, :]
    velocity = kin_ref[state_rows - 3 :, :] + acceleration
    state[...] = jnp.zeros_like(state)
    state[0:3, :] = kin_ref[0:3, :] + velocity
    state[3 : state_rows - 3, :] = kin_ref[6:, :]
    state[state_rows - 3 : state_rows, :] = velocity
    staying = dir_ref[...] == 13
    stayed_ref[...] = jnp.where(staying, state[0:state_rows, :], 0.0)
    target = jnp.where(staying, -1, dir_ref[...] * SLOT_ROWS + slot_ref[...])
    row_id = lax.broadcasted_iota(jnp.int32, (27 * SLOT_ROWS, particles), 0)
    picker = jnp.where(row_id == target, 1.0, 0.0)
    leaving_ref[...] = dot_nt(picker, state[...], HIGHEST).reshape(leaving_ref.shape)


def neighbours():
    sizes = [lax.axis_size(axis) for axis in AXES]
    here = [lax.axis_index(axis) for axis in AXES]
    for q in range(27):
        if q == 13:
            continue
        there = [i + s for i, s in zip(here, (q // 9 - 1, q // 3 % 3 - 1, q % 3 - 1))]
        inside = functools.reduce(
            jnp.logical_and, [jnp.logical_and(t >= 0, t < n) for t, n in zip(there, sizes)]
        )
        yield q, tuple(there), inside


def exchange_kernel(outbox_ref, inbox_ref, send_sems, recv_sems):
    barrier = pltpu.get_barrier_semaphore()
    around = list(neighbours())

    def copy(q, there):
        return pltpu.make_async_remote_copy(
            src_ref=outbox_ref.at[q],
            dst_ref=inbox_ref.at[26 - q],
            send_sem=send_sems.at[q],
            recv_sem=recv_sems.at[26 - q],
            device_id=there,
            device_id_type=MESH,
        )

    def arrival(q, there):
        return pltpu.make_async_remote_copy(
            src_ref=outbox_ref.at[q],
            dst_ref=inbox_ref.at[q],
            send_sem=send_sems.at[q],
            recv_sem=recv_sems.at[q],
            device_id=there,
            device_id_type=MESH,
        )

    for q, there, inside in around:

        @pl.when(inside)
        def _():
            pl.semaphore_signal(barrier, inc=1, device_id=there, device_id_type=MESH)

    blank = jnp.zeros(inbox_ref.shape[1:], inbox_ref.dtype)
    inbox_ref[13] = blank
    for q, there, inside in around:

        @pl.when(jnp.logical_not(inside))
        def _():
            inbox_ref[q] = blank

    peers = 1
    for axis in AXES:
        i, n = lax.axis_index(axis), lax.axis_size(axis)
        peers = peers * (1 + jnp.where(i > 0, 1, 0) + jnp.where(i < n - 1, 1, 0))
    pl.semaphore_wait(barrier, peers - 1)

    for q, there, inside in around:

        @pl.when(inside)
        def _():
            copy(q, there).start()

    for q, there, inside in around:

        @pl.when(inside)
        def _():
            arrival(q, there).wait_recv()
            copy(q, there).wait_send()


def shifted(value, axis, steps):
    count = lax.axis_size(axis)
    first, last = (max(0, -steps), min(count, count - steps))
    return lax.ppermute(value, axis, [(source, source + steps) for source in range(first, last)])


def exchange(outbox, collective_id):
    if KERNEL_EXCHANGE:
        return pl.pallas_call(
            exchange_kernel,
            name="exchange" + str(collective_id),
            out_shape=jax.ShapeDtypeStruct(outbox.shape, outbox.dtype),
            in_specs=[pl.BlockSpec(memory_space=pltpu.VMEM)],
            out_specs=pl.BlockSpec(memory_space=pltpu.VMEM),
            scratch_shapes=[pltpu.SemaphoreType.DMA((27,)), pltpu.SemaphoreType.DMA((27,))],
            compiler_params=pltpu.CompilerParams(
                collective_id=collective_id, has_side_effects=True
            ),
        )(outbox)
    box = outbox.reshape((3, 3, 3) + outbox.shape[1:])
    for dim, axis in enumerate(AXES):
        low, middle, high = [lax.index_in_dim(box, i, dim, keepdims=False) for i in range(3)]
        box = jnp.stack([shifted(high, axis, 1), middle, shifted(low, axis, -1)], axis=dim)
    return box.reshape(outbox.shape)


def whole_spec(array):
    return pl.BlockSpec(array.shape, lambda i, n=array.ndim: (0,) * n)


def round_spec(array, r):
    return pl.BlockSpec((None,) + array.shape[1:], lambda i, n=array.ndim: (r,) + (0,) * (n - 1))


def call(kernel, name, operands, specs, outs, scratch):
    return pl.pallas_call(
        kernel,
        name=name,
        grid=(1,),
        in_specs=specs,
        out_specs=[whole_spec(o) for o in outs],
        out_shape=outs,
        scratch_shapes=scratch,
    )(*operands)


def on_device(
    kinematics,
    pair_offsets,
    pair_index,
    neighbour_count,
    send_rows,
    migrate_dir,
    migrate_slot,
    enc_node_w1,
    enc_node_w2,
    enc_edge_w1,
    enc_edge_w2,
    edge_w1,
    edge_w2,
    node_w1,
    node_w2,
    edge_gain,
    node_gain,
    dec_w1,
    dec_w2,
):
    width = enc_node_w2.shape[1]
    pair_slots, particles = pair_index.shape
    ghost_count = send_rows.shape[1]
    state_rows = kinematics.shape[0]
    rounds = edge_w1.shape[0]
    ghost_rows = 27 * ghost_count
    count = neighbour_count.reshape(1, particles)
    gains = (edge_gain.reshape(rounds, 1, width), node_gain.reshape(rounds, 1, width))
    latent_shape = jax.ShapeDtypeStruct((width, particles), BF16)
    box_shape = jax.ShapeDtypeStruct((27, ghost_count, width), BF16)

    operands = (
        kinematics, pair_offsets, send_rows, enc_node_w1, enc_node_w2, enc_edge_w1, enc_edge_w2,
    )
    latent, edge_latent, send_hot, outbox = call(
        encode_kernel,
        "encode",
        operands,
        [whole_spec(a) for a in operands],
        [
            latent_shape,
            jax.ShapeDtypeStruct((pair_slots, width, particles), BF16),
            jax.ShapeDtypeStruct((ghost_rows, particles), BF16),
            box_shape,
        ],
        [
            pltpu.VMEM((width, width), F32),
            pltpu.VMEM((width, particles), F32),
            pltpu.VMEM((4, width, particles), F32),
        ],
    )
    scratch = [
        pltpu.VMEM((width, particles + ghost_rows), BF16),
        pltpu.VMEM((width, 2 * width), BF16),
    ]
    for r in range(rounds):
        ghosts = exchange(outbox, 0)
        params = (edge_w1, edge_w2, node_w1, node_w2) + gains
        param_specs = [round_spec(a, r) for a in params]
        if r < rounds - 1:
            operands = (latent, ghosts, edge_latent, pair_index, count, send_hot)
            latent, outbox = call(
                round_kernel,
                "round",
                operands + params,
                [whole_spec(a) for a in operands] + param_specs,
                [latent_shape, box_shape],
                scratch,
            )
        else:
            operands = (latent, ghosts, edge_latent, pair_index, count)
            tail = (
                kinematics,
                migrate_dir.reshape(1, particles),
                migrate_slot.reshape(1, particles),
                dec_w1,
                dec_w2,
            )
            stayed, leaving = call(
                last_kernel,
                "last",
                operands + params + tail,
                [whole_spec(a) for a in operands] + param_specs + [whole_spec(a) for a in tail],
                [
                    jax.ShapeDtypeStruct((state_rows, particles), F32),
                    jax.ShapeDtypeStruct((27, SLOT_ROWS, width), F32),
                ],
                scratch + [pltpu.VMEM((width, particles), F32), pltpu.VMEM((8, width), F32)],
            )
    landed = exchange(leaving, 1)
    arrived = landed[:, :MIG, :state_rows].reshape(27 * MIG, state_rows).T
    return (stayed, arrived)


def solution(mesh):
    split = ("gx", "gy", "gz")
    return jax.shard_map(
        on_device,
        mesh=mesh,
        in_specs=(
            P(None, split),
            P(None, None, split),
            P(None, split),
            P(split),
            P(None, split),
            P(split),
            P(split),
        )
        + (P(),) * 12,
        out_specs=(P(None, split), P(None, split)),
        check_vma=False,
    )
```

```python
import functools

import jax
import jax.numpy as jnp
from jax import lax
from jax.experimental import pallas as pl
from jax.experimental.pallas import tpu as pltpu
from jax.sharding import PartitionSpec as P

MIG = 4
SLOT_ROWS = 8

norm_eps = 1e-05
F32 = jnp.float32
BF16 = jnp.bfloat16
HIGHEST = lax.Precision.HIGHEST
MESH = pl.DeviceIdType.MESH
AXES = ("gx", "gy", "gz")


def dot(a, b, precision=None):
    return jnp.dot(a, b, preferred_element_type=F32, precision=precision)


def dot_nt(a, b, precision=None):
    return lax.dot_general(
        a, b, (((1,), (1,)), ((), ())), preferred_element_type=F32, precision=precision
    )


def turned(weight):
    return weight.astype(F32).T.astype(weight.dtype)


def normed(values):
    center = values - jnp.mean(values, axis=0, keepdims=True)
    spread = jnp.mean(center * center, axis=0, keepdims=True)
    return center, lax.rsqrt(spread + norm_eps)


def as_column(row, lanes):
    width = row.shape[1]
    square = jnp.broadcast_to(row, (width, width)).T
    return jnp.broadcast_to(square[:, 0:1], (width, lanes))


def fill_outbox(send_hot, latent, outbox_ref):
    outbox_ref[...] = dot_nt(send_hot, latent).astype(BF16).reshape(outbox_ref.shape)


def encode_nodes(kin_ref, send_ref, node_w1, node_w2, latent_ref, hot_ref, square, wide):
    particles = kin_ref.shape[1]
    directions, ghost_count = send_ref.shape
    features = node_w1.shape[0]
    square[...] = jnp.zeros_like(square)
    wide[...] = jnp.zeros_like(wide)
    square[0:features, :] = node_w1[...]
    wide[0:features, :] = kin_ref[3:, :]
    hidden = jnp.maximum(dot(square[...].T, wide[...], HIGHEST), 0.0).astype(BF16)
    center, scale = normed(dot(turned(node_w2[...]), hidden))
    latent_ref[...] = (center * scale).astype(BF16)

    rows = lax.broadcasted_iota(jnp.int32, (ghost_count, ghost_count), 0)
    lanes = lax.broadcasted_iota(jnp.int32, (ghost_count, ghost_count), 1)
    unit = (rows == lanes).astype(F32)
    wanted = dot_nt(unit, send_ref[...].astype(F32), HIGHEST)
    position = lax.broadcasted_iota(jnp.int32, (ghost_count, particles), 1).astype(F32)
    for q in range(directions):
        near = jnp.abs(wanted[:, q : q + 1] - position) < 0.5
        hot_ref[q * ghost_count : (q + 1) * ghost_count, :] = jnp.where(near, 1.0, 0.0).astype(BF16)


def encode_edges(off_ref, index_ref, edge_w1, edge_w2, edge_ref, pair_hot, square, columns):
    width = edge_w2.shape[1]
    particles = off_ref.shape[2]
    pair_slots, rows = pair_hot.shape[:2]
    square[0:4, :] = edge_w1[...]
    first = square[...].T
    for c in range(4):
        columns[c] = jnp.broadcast_to(first[:, c : c + 1], (width, particles))
    second = turned(edge_w2[...])
    row_id = lax.broadcasted_iota(jnp.int32, (rows, particles), 0)

    def one_slot(k, carry):
        x = off_ref[0, pl.ds(k, 1), :]
        y = off_ref[1, pl.ds(k, 1), :]
        z = off_ref[2, pl.ds(k, 1), :]
        pre = columns[0] * x + columns[1] * y + columns[2] * z
        pre = pre + columns[3] * (x * x + y * y + z * z)
        mid = jnp.maximum(pre, 0.0).astype(BF16)
        center, scale = normed(dot(second, mid))
        edge_ref[k] = (center * scale).astype(BF16)
        pair_hot[k] = jnp.where(row_id == index_ref[pl.ds(k, 1), :], 1.0, 0.0).astype(BF16)
        return carry

    lax.fori_loop(0, pair_slots, one_slot, 0, unroll=4)


def prepare(latent_ref, edge_w1, edge_w2, extended, joined):
    width, particles = latent_ref.shape
    latent = latent_ref[...]
    extended[:, :particles] = latent
    joined[:, :width] = turned(edge_w1[:width, :])
    joined[:, width:] = turned(edge_w1[2 * width :, :])
    received = dot(turned(edge_w1[width : 2 * width, :]), latent)
    return latent, received, turned(edge_w2[...])


def update_latent(
    ready, ghost_ref, edge_ref, pair_hot, count_ref, node_w1, node_w2, edge_gain, node_gain,
    extended, joined,
):
    latent, received, second = ready
    width, particles = latent.shape
    pair_slots = edge_ref.shape[0]
    ghosts = ghost_ref[...].reshape(-1, width)
    diagonal = lax.broadcasted_iota(jnp.int32, (width, width), 0) == lax.broadcasted_iota(
        jnp.int32, (width, width), 1
    )
    unit = jnp.where(diagonal, 1.0, 0.0).astype(BF16)
    extended[:, particles:] = dot_nt(unit, ghosts).astype(BF16)
    count = count_ref[...]

    def one_slot(k, total):
        sender = dot(extended[...], pair_hot[k]).astype(BF16)
        both = jnp.concatenate([edge_ref[k], sender], axis=0)
        hidden = jnp.maximum(dot(joined[...], both) + received, 0.0).astype(BF16)
        center, scale = normed(dot(second, hidden))
        return total + center * jnp.where(k < count, scale, 0.0)

    total = lax.fori_loop(
        0, pair_slots, one_slot, jnp.zeros((width, particles), F32), unroll=4
    )
    aggregate = (total * as_column(edge_gain[...], particles)).astype(BF16)
    pre = dot(turned(node_w1[:width, :]), latent) + dot(turned(node_w1[width:, :]), aggregate)
    center, scale = normed(dot(turned(node_w2[...]), jnp.maximum(pre, 0.0).astype(BF16)))
    update = center * scale * as_column(node_gain[...], particles)
    return (latent.astype(F32) + update).astype(BF16)


def finish(
    latent, kin_ref, dir_ref, slot_ref, dec_w1, dec_w2, stayed_ref, leaving_ref, state, reading
):
    state_rows, particles = kin_ref.shape
    hidden = jnp.maximum(dot(turned(dec_w1[...]), latent), 0.0).astype(BF16)
    reading[...] = jnp.zeros_like(reading)
    reading[0:3, :] = dec_w2[...]
    acceleration = dot(reading[...], hidden.astype(F32), HIGHEST)[0:3, :]
    velocity = kin_ref[state_rows - 3 :, :] + acceleration
    state[...] = jnp.zeros_like(state)
    state[0:3, :] = kin_ref[0:3, :] + velocity
    state[3 : state_rows - 3, :] = kin_ref[6:, :]
    state[state_rows - 3 : state_rows, :] = velocity
    staying = dir_ref[...] == 13
    stayed_ref[...] = jnp.where(staying, state[0:state_rows, :], 0.0)
    target = jnp.where(staying, -1, dir_ref[...] * SLOT_ROWS + slot_ref[...])
    row_id = lax.broadcasted_iota(jnp.int32, (27 * SLOT_ROWS, particles), 0)
    picker = jnp.where(row_id == target, 1.0, 0.0)
    leaving_ref[...] = dot_nt(picker, state[...], HIGHEST).reshape(leaving_ref.shape)


def neighbours():
    sizes = [lax.axis_size(axis) for axis in AXES]
    here = [lax.axis_index(axis) for axis in AXES]
    for q in range(27):
        if q == 13:
            continue
        there = [i + s for i, s in zip(here, (q // 9 - 1, q // 3 % 3 - 1, q % 3 - 1))]
        inside = functools.reduce(
            jnp.logical_and, [jnp.logical_and(t >= 0, t < n) for t, n in zip(there, sizes)]
        )
        yield q, tuple(there), inside


def enter(around):
    barrier = pltpu.get_barrier_semaphore()
    for q, there, inside in around:

        @pl.when(inside)
        def _():
            pl.semaphore_signal(barrier, inc=1, device_id=there, device_id_type=MESH)

    peers = 1
    for axis in AXES:
        i, n = lax.axis_index(axis), lax.axis_size(axis)
        peers = peers * (1 + jnp.where(i > 0, 1, 0) + jnp.where(i < n - 1, 1, 0))
    return barrier, peers - 1


def send(around, outbox_ref, inbox_ref, send_sems, recv_sems):
    for q, there, inside in around:

        @pl.when(inside)
        def _():
            pltpu.make_async_remote_copy(
                src_ref=outbox_ref.at[q],
                dst_ref=inbox_ref.at[26 - q],
                send_sem=send_sems.at[q],
                recv_sem=recv_sems.at[26 - q],
                device_id=there,
                device_id_type=MESH,
            ).start()


def land(around, outbox_ref, inbox_ref, send_sems, recv_sems):
    for q, there, inside in around:

        @pl.when(inside)
        def _():
            copy = pltpu.make_async_remote_copy(
                src_ref=outbox_ref.at[q],
                dst_ref=inbox_ref.at[q],
                send_sem=send_sems.at[q],
                recv_sem=recv_sems.at[q],
                device_id=there,
                device_id_type=MESH,
            )
            copy.wait_recv()
            copy.wait_send()


def step_kernel(
    kin_ref, off_ref, index_ref, count_ref, send_ref, dir_ref, slot_ref, enc_node_w1, enc_node_w2,
    enc_edge_w1, enc_edge_w2, edge_w1, edge_w2, node_w1, node_w2, edge_gain, node_gain, dec_w1,
    dec_w2, stayed_ref, arrived_ref, latent_ref, edge_ref, send_hot, pair_hot, outbox, inbox,
    leaving, landed, send_sems, recv_sems, square, wide, columns, extended, joined, reading,
):
    around = list(neighbours())
    for r in range(inbox.shape[0]):
        inbox[r] = jnp.zeros(inbox.shape[1:], inbox.dtype)
    landed[...] = jnp.zeros_like(landed)
    barrier, peers = enter(around)
    encode_nodes(
        kin_ref, send_ref, enc_node_w1, enc_node_w2, latent_ref, send_hot, square, wide
    )
    fill_outbox(send_hot[...], latent_ref[...], outbox.at[0])
    pl.semaphore_wait(barrier, peers)
    rounds = edge_w1.shape[0]
    for r in range(rounds):
        path = (outbox.at[r], inbox.at[r], send_sems.at[r], recv_sems.at[r])
        send(around, *path)
        if r == 0:
            encode_edges(
                off_ref, index_ref, enc_edge_w1, enc_edge_w2, edge_ref, pair_hot, square, columns
            )
        ready = prepare(latent_ref, edge_w1.at[r], edge_w2.at[r], extended, joined)
        land(around, *path)
        latent = update_latent(
            ready, inbox.at[r], edge_ref, pair_hot, count_ref, node_w1.at[r], node_w2.at[r],
            edge_gain.at[r : r + 1], node_gain.at[r : r + 1], extended, joined,
        )
        latent_ref[...] = latent
        if r < rounds - 1:
            fill_outbox(send_hot[...], latent, outbox.at[r + 1])
    finish(
        latent, kin_ref, dir_ref, slot_ref, dec_w1, dec_w2, stayed_ref, leaving, wide, reading
    )
    path = (leaving, landed, send_sems.at[rounds], recv_sems.at[rounds])
    send(around, *path)
    land(around, *path)
    state_rows = kin_ref.shape[0]
    turned_rows = landed[...].reshape(27 * SLOT_ROWS, landed.shape[2])
    spread = lax.broadcasted_iota(jnp.int32, (27 * MIG, 27 * SLOT_ROWS), 0)
    source = lax.broadcasted_iota(jnp.int32, (27 * MIG, 27 * SLOT_ROWS), 1)
    lane = spread // MIG * SLOT_ROWS + spread % MIG
    compact = jnp.where(lane == source, 1.0, 0.0)
    unit_rows = lax.broadcasted_iota(jnp.int32, (landed.shape[2],) * 2, 0)
    unit_lanes = lax.broadcasted_iota(jnp.int32, (landed.shape[2],) * 2, 1)
    unit = jnp.where(unit_rows == unit_lanes, 1.0, 0.0)
    across = dot_nt(unit, turned_rows, HIGHEST)
    arrived_ref[...] = dot_nt(across, compact, HIGHEST)[0:state_rows, :]


def on_device(
    kinematics,
    pair_offsets,
    pair_index,
    neighbour_count,
    send_rows,
    migrate_dir,
    migrate_slot,
    enc_node_w1,
    enc_node_w2,
    enc_edge_w1,
    enc_edge_w2,
    edge_w1,
    edge_w2,
    node_w1,
    node_w2,
    edge_gain,
    node_gain,
    dec_w1,
    dec_w2,
):
    width = enc_node_w2.shape[1]
    pair_slots, particles = pair_index.shape
    ghost_count = send_rows.shape[1]
    state_rows = kinematics.shape[0]
    rounds = edge_w1.shape[0]
    ghost_rows = 27 * ghost_count
    total_rows = particles + ghost_rows
    operands = (
        kinematics, pair_offsets, pair_index, neighbour_count.reshape(1, particles), send_rows,
        migrate_dir.reshape(1, particles), migrate_slot.reshape(1, particles), enc_node_w1,
        enc_node_w2, enc_edge_w1, enc_edge_w2, edge_w1, edge_w2, node_w1, node_w2, edge_gain,
        node_gain, dec_w1, dec_w2,
    )
    vmem = pl.BlockSpec(memory_space=pltpu.VMEM)
    return tuple(
        pl.pallas_call(
            step_kernel,
            name="step",
            in_specs=[vmem] * len(operands),
            out_specs=[vmem, vmem],
            out_shape=[
                jax.ShapeDtypeStruct((state_rows, particles), F32),
                jax.ShapeDtypeStruct((state_rows, 27 * MIG), F32),
            ],
            scratch_shapes=[
                pltpu.VMEM((width, particles), BF16),
                pltpu.VMEM((pair_slots, width, particles), BF16),
                pltpu.VMEM((ghost_rows, particles), BF16),
                pltpu.VMEM((pair_slots, total_rows, particles), BF16),
                pltpu.VMEM((rounds, 27, ghost_count, width), BF16),
                pltpu.VMEM((rounds, 27, ghost_count, width), BF16),
                pltpu.VMEM((27, SLOT_ROWS, width), F32),
                pltpu.VMEM((27, SLOT_ROWS, width), F32),
                pltpu.SemaphoreType.DMA((rounds + 1, 27)),
                pltpu.SemaphoreType.DMA((rounds + 1, 27)),
                pltpu.VMEM((width, width), F32),
                pltpu.VMEM((width, particles), F32),
                pltpu.VMEM((4, width, particles), F32),
                pltpu.VMEM((width, total_rows), BF16),
                pltpu.VMEM((width, 2 * width), BF16),
                pltpu.VMEM((8, width), F32),
            ],
            compiler_params=pltpu.CompilerParams(collective_id=0, has_side_effects=True),
        )(*operands)
    )


def solution(mesh):
    split = ("gx", "gy", "gz")
    return jax.shard_map(
        on_device,
        mesh=mesh,
        in_specs=(
            P(None, split),
            P(None, None, split),
            P(None, split),
            P(split),
            P(None, split),
            P(split),
            P(split),
        )
        + (P(),) * 12,
        out_specs=(P(None, split), P(None, split)),
        check_vma=False,
    )
```
